32 devices in a mesh: gx: 2 (over core), gy: 16 (over z, y, x).
Axes of the slice: x: 2, y: 2, z: 4, core: 2. Of those that a mesh axis runs over, the one named last changes fastest.
Arguments:
- data: float32 [32, 256, 128], P('gx', 'gy'), may hold values from -6 to 6
- precond: float32 [32, 256, 128], P('gx', 'gy'), may hold values from 0.5 to 2
- psf: float32 [2, 16, 17, 17, 17], P('gx', 'gy'), may hold values from -0.05 to 0.05
Outputs:
- model: float32 [32, 256, 128], P('gx', 'gy')
- residual: float32 [32, 256, 128], P('gx', 'gy')
The draws below stay inside these ranges and needn't reach their ends.
All inputs are finite; a program needn't handle non-finite values.
Results may differ from the reference program's by a relative error of at most 0.0003.
Values sent between devices are 32-bit elements; how exact they have to be, the bound alone decides.
A program may use at most 64 MiB of HBM per device.

```python
import math
import jax
import jax.numpy as jnp
from jax import lax

CX = 16
CY = 16
NZ = 128
PSF = 17
ITERS = 2
NX = 32
NY = 256
N_GX = 2
N_GY = 16


def block_levels(own_key, dims, pieces, smallest, largest):
    def one(position, shards_of):
        steps = jax.random.uniform(jax.random.fold_in(jax.random.fold_in(own_key, 6), position), (shards_of,), jnp.float32, smallest / len(pieces), largest / len(pieces))
        return jnp.repeat(jnp.exp(steps), dims[position] // shards_of).reshape((-1,) + (1,) * (len(dims) - position - 1))

    loudness = one(*pieces[0])
    for cut in pieces[1:]:
        loudness = loudness * one(*cut)
    return loudness


def centred(stream_key, extent, spread, limit, cuts=(), kind=jnp.bfloat16):
    result = spread * jax.random.normal(stream_key, extent, jnp.float32)
    if cuts:
        result = result * block_levels(stream_key, extent, cuts, -0.22, 0.18)
    return jnp.clip(result, -limit, limit).astype(kind)


def setup_inputs(seed: int = 0) -> dict:
    keys = jax.random.split(jax.random.key(seed), 4)
    return {
        "data": centred(keys[0], (NX, NY, NZ), 1.0, 6.0, ((0, 2), (1, 16)), jnp.float32),
        "precond": jnp.clip(jnp.exp(math.log(2.0) - 1.3862944 * jax.random.uniform(keys[1], (NX, NY, NZ), jnp.float32) ** block_levels(keys[1], (NX, NY, NZ), ((0, 2), (1, 16)), -0.2, 0.2)), 0.5, 2.0),
        "psf": centred(keys[2], (N_GX, N_GY, PSF, PSF, PSF), 0.008, 0.05, ((0, 2), (1, 16)), jnp.float32),
    }


relaxation = 0.7


def node_spectrum(kernel, length_x, length_y, length_z, half):
    width = kernel.shape[0]
    flipped = kernel[::-1, ::-1, ::-1]
    placed = jnp.zeros((length_x, length_y, length_z), kernel.dtype).at[:width, :width, :width].set(flipped)
    return jnp.fft.fftn(jnp.roll(placed, (-half, -half, -half), axis=(0, 1, 2)))


def apply_operator(field, psf):
    width = psf.shape[2]
    half = width // 2
    padded = jnp.pad(field, half)
    length_x = CX + 2 * half
    length_y = CY + 2 * half
    length_z = NZ + 2 * half
    along_x = (jnp.arange(CX, dtype=jnp.float32) + 0.5) / CX
    along_y = (jnp.arange(CY, dtype=jnp.float32) + 0.5) / CY

    def one_tile(index):
        row = (index // N_GY).astype(jnp.int32)
        column = (index % N_GY).astype(jnp.int32)
        row_next = jnp.minimum(row + 1, N_GX - 1).astype(jnp.int32)
        column_next = jnp.minimum(column + 1, N_GY - 1).astype(jnp.int32)
        start = (row * CX).astype(jnp.int32)
        begin = (column * CY).astype(jnp.int32)
        region = lax.dynamic_slice(padded, (start, begin, jnp.int32(0)), (length_x, length_y, length_z))
        region_spectrum = jnp.fft.fftn(region)
        nodes = ((row, column, (1.0 - along_x)[:, None] * (1.0 - along_y)[None, :]),
                 (row_next, column, along_x[:, None] * (1.0 - along_y)[None, :]),
                 (row, column_next, (1.0 - along_x)[:, None] * along_y[None, :]),
                 (row_next, column_next, along_x[:, None] * along_y[None, :]))
        total = jnp.zeros((CX, CY, NZ), field.dtype)
        for node_row, node_column, weight in nodes:
            kernel = psf[node_row, node_column]
            spectrum = node_spectrum(kernel, length_x, length_y, length_z, half)
            full = jnp.real(jnp.fft.ifftn(region_spectrum * spectrum))
            inner = full[half:half + CX, half:half + CY, half:half + NZ]
            total = total + weight[:, :, None].astype(field.dtype) * inner.astype(field.dtype)
        return total

    tiles = lax.map(one_tile, jnp.arange(N_GX * N_GY, dtype=jnp.int32))
    tiles = tiles.reshape(N_GX, N_GY, CX, CY, NZ).transpose(0, 2, 1, 3, 4).reshape(NX, NY, NZ)
    return field + tiles


def reference(data, precond, psf):
    model = precond * data
    residual = data
    for sweep_index in range(ITERS):
        residual = data - apply_operator(model, psf)
        model = model + relaxation * precond * residual
    return model, residual
```

```python
import functools
import math

import jax
import jax.numpy as jnp
import numpy as np
from jax import lax
from jax.experimental import pallas as pl
from jax.experimental.pallas import tpu as pltpu
from jax.sharding import PartitionSpec as P

ITERS = 2
relaxation = 0.7
exact = lax.Precision.HIGHEST
LANES = 128
SUB = 8


def times_phase(value, turn, size, sign):
    if value is None:
        return None
    re, im = value
    turn = (sign * turn) % size
    eighth = 8 * turn
    if eighth == 0:
        return value
    if eighth == 2 * size:
        return (-im, re)
    if eighth == 4 * size:
        return (-re, -im)
    if eighth == 6 * size:
        return (im, -re)
    angle = 2.0 * math.pi * turn / size
    cosine, sine = math.cos(angle), math.sin(angle)
    if eighth % size == 0:
        root = math.sqrt(0.5)
        first, second = (re - im) * root, (re + im) * root
        if eighth == size:
            return (first, second)
        if eighth == 3 * size:
            return (-second, first)
        if eighth == 5 * size:
            return (-first, -second)
        return (second, -first)
    return (re * cosine - im * sine, re * sine + im * cosine)


def plus(a, b):
    if a is None:
        return b
    if b is None:
        return a
    return (a[0] + b[0], a[1] + b[1])


def minus(a, b):
    if b is None:
        return a
    if a is None:
        return (-b[0], -b[1])
    return (a[0] - b[0], a[1] - b[1])


def transform(values, sign, wanted):
    size = len(values)
    if all(v is None for v in values):
        return [None] * wanted
    if size == 1:
        return list(values)
    half = size // 2
    if size % 2:
        raise ValueError("length")
    even = transform(values[0::2], sign, min(half, wanted))
    odd = transform(values[1::2], sign, min(half, wanted))
    odd = [times_phase(v, k, size, sign) for k, v in enumerate(odd)]
    low = [plus(a, b) for a, b in zip(even, odd)]
    high = [minus(a, b) for a, b in zip(even, odd)]
    return (low + high)[:wanted]


def tables(depth, width):
    half = width // 2
    length = depth + 2 * half
    count = length // 2 + 1
    k = np.arange(count)
    field = np.zeros((depth, 2 * LANES))
    turns = (np.arange(depth)[:, None] + half) * k[None, :] % length
    angle = turns * (2.0 * np.pi / length)
    field[:, :count] = np.cos(angle)
    field[:, LANES : LANES + count] = -np.sin(angle)
    kernel = np.zeros((LANES, 2 * LANES))
    angle = np.arange(width)[:, None] * k[None, :] % length * (2.0 * np.pi / length)
    kernel[:width, :count] = np.cos(angle)
    kernel[:width, LANES : LANES + count] = np.sin(angle)
    back = np.zeros((2 * LANES, depth))
    weight = np.where((k == 0) | (2 * k == length), 1.0, 2.0) / length
    angle = k[:, None] * np.arange(depth)[None, :] % length * (2.0 * np.pi / length)
    back[:count] = weight[:, None] * np.cos(angle)
    back[LANES : LANES + count] = -weight[:, None] * np.sin(angle)
    return field.astype(np.float32), kernel.astype(np.float32), back


def spectra_kernel(width, region_x, region_y, rows, psf_ref, table_ref, g_ref, k1r, k1i, k2r, k2i):
    for b in range(width):
        both = jnp.dot(
            psf_ref[pl.ds(b * rows, rows), :], table_ref[...],
            precision=exact, preferred_element_type=jnp.float32,
        )
        k1r[pl.ds(b * rows, rows), :] = both[:, :LANES]
        k1i[pl.ds(b * rows, rows), :] = both[:, LANES:]

    @pl.loop(0, rows // SUB)
    def _(tile):
        at = lambda i: pl.ds(pl.multiple_of(i * rows + tile * SUB, SUB), SUB)
        values = [(k1r[at(b), :], k1i[at(b), :]) for b in range(width)]
        values += [None] * (region_y - width)
        for ky, (re, im) in enumerate(transform(values, 1, region_y)):
            k2r[at(ky), :] = re
            k2i[at(ky), :] = im

    @pl.loop(0, 4)
    def _(node):
        @pl.loop(0, region_y // SUB)
        def _(tile):
            at = lambda a: pl.ds(tile * SUB * rows + node * width + a, SUB, stride=rows)
            values = [(k2r[at(a), :], k2i[at(a), :]) for a in range(width)]
            values += [None] * (region_x - width)
            for kx, (re, im) in enumerate(transform(values, 1, region_x)):
                to = pl.ds(pl.multiple_of(kx * region_y + tile * SUB, SUB), SUB)
                g_ref[node, 0, to, :] = re
                g_ref[node, 1, to, :] = im


def apply_kernel(
    count_x, count_y, half,
    region_ref, data_ref, precond_ref, g_hbm, field_ref, back_ref,
    model_ref, residual_ref,
    g_ref, zr, zi, yr, yi, vx, ur, ui, w_ref, o_ref, sem,
):
    region_x, region_y = count_x + 2 * half, count_y + 2 * half
    fetch = pltpu.make_async_copy(g_hbm, g_ref, sem)
    fetch.start()
    block = 128
    for start in range(0, region_x * region_y, block):
        both = jnp.dot(
            region_ref[pl.ds(start, block), :], field_ref[...],
            precision=exact, preferred_element_type=jnp.float32,
        )
        zr[pl.ds(start, block), :] = both[:, :LANES]
        zi[pl.ds(start, block), :] = both[:, LANES:]

    @pl.loop(0, region_x // SUB)
    def _(tile):
        at = lambda y: pl.ds(tile * SUB * region_y + y, SUB, stride=region_y)
        values = [(zr[at(y), :], zi[at(y), :]) for y in range(region_y)]
        for ky, (re, im) in enumerate(transform(values, -1, region_y)):
            to = pl.ds(pl.multiple_of(ky * region_x + tile * SUB, SUB), SUB)
            yr[to, :] = re
            yi[to, :] = im

    fetch.wait()

    @pl.loop(0, region_y // SUB)
    def _(tile):
        at = lambda x: pl.ds(tile * SUB * region_x + x, SUB, stride=region_x)
        values = [(yr[at(x), :], yi[at(x), :]) for x in range(region_x)]
        for kx, (re, im) in enumerate(transform(values, -1, region_x)):
            vx[0, kx] = re
            vx[1, kx] = im

        @pl.loop(0, 2)
        def _(j):
            parts = []
            for i in range(2):
                values = []
                for kx in range(region_x):
                    to = pl.ds(pl.multiple_of(kx * region_y + tile * SUB, SUB), SUB)
                    gr, gi = g_ref[2 * j + i, 0, to, :], g_ref[2 * j + i, 1, to, :]
                    vr, vi = vx[0, kx], vx[1, kx]
                    values.append((vr * gr - vi * gi, vr * gi + vi * gr))
                parts.append(transform(values, 1, count_x))
            for x in range(count_x):
                s = (x + 0.5) / count_x
                to = pl.ds(pl.multiple_of(x * region_y + tile * SUB, SUB), SUB)
                (ar, ai), (br, bi) = parts[0][x], parts[1][x]
                ur[j, to, :] = (1.0 - s) * ar + s * br
                ui[j, to, :] = (1.0 - s) * ai + s * bi

    @pl.loop(0, count_x // SUB)
    def _(tile):
        parts = []
        for j in range(2):
            at = lambda ky: pl.ds(tile * SUB * region_y + ky, SUB, stride=region_y)
            values = [(ur[j, at(ky), :], ui[j, at(ky), :]) for ky in range(region_y)]
            parts.append(transform(values, 1, count_y))
        for y in range(count_y):
            t = (y + 0.5) / count_y
            to = pl.ds(pl.multiple_of(y * count_x + tile * SUB, SUB), SUB)
            (ar, ai), (br, bi) = parts[0][y], parts[1][y]
            w_ref[to, :LANES] = (1.0 - t) * ar + t * br
            w_ref[to, LANES:] = (1.0 - t) * ai + t * bi

    o_ref[...] = jnp.dot(
        w_ref[...], back_ref[...], precision=exact, preferred_element_type=jnp.float32
    )
    for x in range(count_x):
        blended = o_ref[pl.ds(x, count_y, stride=count_x), :]
        model = region_ref[pl.ds((x + half) * region_y + half, count_y), :]
        residual = data_ref[x] - (model + blended)
        residual_ref[x] = residual
        model_ref[x] = model + relaxation * precond_ref[x] * residual


def padded_2(shard, sides, width):
    for axis, dim in sides:
        size, length = (lax.axis_size(axis), shard.shape[dim])
        up = [(i, (i + 1) % size) for i in range(size - 1)]
        down = [(j, i) for i, j in up]
        last = lax.slice_in_dim(shard, length - width, length, axis=dim)
        leading = lax.slice_in_dim(shard, 0, width, axis=dim)
        before = lax.ppermute(last, axis, up)
        after = lax.ppermute(leading, axis, down)
        shard = jnp.concatenate([before, shard, after], axis=dim)
    return shard


def passed_along(shard, axis, by):
    length = lax.axis_size(axis)
    pairs = [(i, i + by) for i in range(length) if 0 <= i + by < length]
    return lax.ppermute(shard, axis, pairs)


def node_kernels(psf):
    own = psf[0, 0]
    last_inline = lax.axis_index("gx") == lax.axis_size("gx") - 1
    last_crossline = lax.axis_index("gy") == lax.axis_size("gy") - 1
    inline = jnp.where(last_inline, own, passed_along(own, "gx", -1))
    pair = jnp.stack([own, inline])
    crossline = jnp.where(last_crossline, pair, passed_along(pair, "gy", -1))
    return jnp.concatenate([pair, crossline])


def local(data, precond, psf):
    count_x, count_y, depth = data.shape
    width = psf.shape[2]
    half = width // 2
    region_x, region_y = count_x + 2 * half, count_y + 2 * half
    field, kernel, back = tables(depth, width)
    back = (back / (region_x * region_y)).astype(np.float32)
    f32 = jnp.float32

    model = precond * data
    nodes = node_kernels(psf)
    rows = -(-4 * width // SUB) * SUB
    arranged = nodes.transpose(2, 0, 1, 3).reshape(width, 4 * width, width)
    arranged = jnp.pad(arranged, ((0, 0), (0, rows - 4 * width), (0, LANES - width)))
    arranged = arranged.reshape(width * rows, LANES)
    spectra = pl.pallas_call(
        functools.partial(spectra_kernel, width, region_x, region_y, rows),
        out_shape=jax.ShapeDtypeStruct((4, 2, region_x * region_y, LANES), f32),
        scratch_shapes=[pltpu.VMEM((width * rows, LANES), f32)] * 2
        + [pltpu.VMEM((region_y * rows, LANES), f32)] * 2,
        compiler_params=pltpu.CompilerParams(vmem_limit_bytes=24 << 20),
        cost_estimate=pl.CostEstimate(flops=10**9, bytes_accessed=10**6, transcendentals=0),
        name="spectra",
    )(arranged, kernel)

    vmem = pl.BlockSpec(memory_space=pltpu.VMEM)
    apply = pl.pallas_call(
        functools.partial(apply_kernel, count_x, count_y, half),
        out_shape=[jax.ShapeDtypeStruct(data.shape, f32)] * 2,
        in_specs=[vmem, vmem, vmem, pl.BlockSpec(memory_space=pl.ANY), vmem, vmem],
        scratch_shapes=[
            pltpu.VMEM((4, 2, region_x * region_y, LANES), f32),
            pltpu.VMEM((region_x * region_y, LANES), f32),
            pltpu.VMEM((region_x * region_y, LANES), f32),
            pltpu.VMEM((region_x * region_y, LANES), f32),
            pltpu.VMEM((region_x * region_y, LANES), f32),
            pltpu.VMEM((2, region_x, SUB, LANES), f32),
            pltpu.VMEM((2, count_x * region_y, LANES), f32),
            pltpu.VMEM((2, count_x * region_y, LANES), f32),
            pltpu.VMEM((count_x * count_y, 2 * LANES), f32),
            pltpu.VMEM((count_x * count_y, LANES), f32),
            pltpu.SemaphoreType.DMA,
        ],
        compiler_params=pltpu.CompilerParams(vmem_limit_bytes=24 << 20),
        name="apply",
    )
    residual = data
    for sweep_index in range(ITERS):
        region = padded_2(model, (("gx", 0), ("gy", 1)), half)
        region = region.reshape(region_x * region_y, depth)
        model, residual = apply(region, data, precond, spectra, field, back)
    return model, residual


def solution(mesh):
    placed = (P("gx", "gy", None), P("gx", "gy", None), P("gx", "gy", None, None, None))
    return jax.shard_map(
        local,
        mesh=mesh,
        in_specs=placed,
        out_specs=(P("gx", "gy", None), P("gx", "gy", None)),
        check_vma=False,
    )
```

```python
import functools
import math

import jax
import jax.numpy as jnp
import numpy as np
from jax import lax
from jax.experimental import pallas as pl
from jax.experimental.pallas import tpu as pltpu
from jax.sharding import PartitionSpec as P

ITERS = 2
relaxation = 0.7
LANES = 128
SUB = 8


def times_phase(value, turn, size, sign):
    if value is None:
        return None
    re, im = value
    turn = (sign * turn) % size
    eighth = 8 * turn
    if eighth == 0:
        return value
    if eighth == 2 * size:
        return (-im, re)
    if eighth == 4 * size:
        return (-re, -im)
    if eighth == 6 * size:
        return (im, -re)
    angle = 2.0 * math.pi * turn / size
    cosine, sine = math.cos(angle), math.sin(angle)
    if eighth % size == 0:
        root = math.sqrt(0.5)
        first, second = (re - im) * root, (re + im) * root
        if eighth == size:
            return (first, second)
        if eighth == 3 * size:
            return (-second, first)
        if eighth == 5 * size:
            return (-first, -second)
        return (second, -first)
    return (re * cosine - im * sine, re * sine + im * cosine)


def plus(a, b):
    if a is None:
        return b
    if b is None:
        return a
    return (a[0] + b[0], a[1] + b[1])


def minus(a, b):
    if b is None:
        return a
    if a is None:
        return (-b[0], -b[1])
    return (a[0] - b[0], a[1] - b[1])


def transform(values, sign, wanted):
    size = len(values)
    if all(v is None for v in values):
        return [None] * wanted
    if size == 1:
        return list(values)
    half = size // 2
    if size % 2:
        raise ValueError("length")
    even = transform(values[0::2], sign, min(half, wanted))
    odd = transform(values[1::2], sign, min(half, wanted))
    odd = [times_phase(v, k, size, sign) for k, v in enumerate(odd)]
    low = [plus(a, b) for a, b in zip(even, odd)]
    high = [minus(a, b) for a, b in zip(even, odd)]
    return (low + high)[:wanted]


def tables(depth, width):
    half = width // 2
    length = depth + 2 * half
    count = length // 2 + 1
    k = np.arange(count)
    field = np.zeros((depth, 2 * LANES))
    turns = (np.arange(depth)[:, None] + half) * k[None, :] % length
    angle = turns * (2.0 * np.pi / length)
    field[:, :count] = np.cos(angle)
    field[:, LANES : LANES + count] = -np.sin(angle)
    kernel = np.zeros((LANES, 2 * LANES))
    angle = np.arange(width)[:, None] * k[None, :] % length * (2.0 * np.pi / length)
    kernel[:width, :count] = np.cos(angle)
    kernel[:width, LANES : LANES + count] = np.sin(angle)
    back = np.zeros((2 * LANES, depth))
    weight = np.where((k == 0) | (2 * k == length), 1.0, 2.0) / length
    angle = k[:, None] * np.arange(depth)[None, :] % length * (2.0 * np.pi / length)
    back[:count] = weight[:, None] * np.cos(angle)
    back[LANES : LANES + count] = -weight[:, None] * np.sin(angle)
    return field, kernel, back


def stacked(table):
    high = jnp.asarray(table, jnp.float32).astype(jnp.bfloat16)
    low = (jnp.asarray(table, jnp.float32) - high.astype(jnp.float32)).astype(jnp.bfloat16)
    return jnp.concatenate([high, high, low])


def product(left, table):
    high = left.astype(jnp.bfloat16)
    low = (left - high.astype(jnp.float32)).astype(jnp.bfloat16)
    left = jnp.concatenate([high, low, high], axis=1)
    return jnp.dot(left, table, preferred_element_type=jnp.float32)


def pitch_of(rows):
    return rows + SUB if rows % (4 * SUB) == 0 else rows


def spectra(width, region_x, region_y, rows, packed, table_ref, g_ref, k1r, k1i, k2r, k2i):
    lanes = packed.shape[1]
    for b in range(width):
        shifted = packed[...]
        if b:
            shifted = pltpu.roll(shifted, lanes - b * width, axis=1)
        both = product(shifted[:, :LANES], table_ref[...])
        k1r[pl.ds(b * rows, rows), :] = both[:, :LANES]
        k1i[pl.ds(b * rows, rows), :] = both[:, LANES:]

    @pl.loop(0, rows // SUB)
    def _(tile):
        at = lambda i: pl.ds(pl.multiple_of(i * rows + tile * SUB, SUB), SUB)
        values = [(k1r[at(b), :], k1i[at(b), :]) for b in range(width)]
        values += [None] * (region_y - width)
        for ky, (re, im) in enumerate(transform(values, 1, region_y)):
            k2r[at(ky), :] = re
            k2i[at(ky), :] = im

    @pl.loop(0, 4)
    def _(node):
        @pl.loop(0, region_y // SUB)
        def _(tile):
            at = lambda a: pl.ds(tile * SUB * rows + node * width + a, SUB, stride=rows)
            values = [(k2r[at(a), :], k2i[at(a), :]) for a in range(width)]
            values += [None] * (region_x - width)
            for kx, (re, im) in enumerate(transform(values, 1, region_x)):
                to = pl.ds(pl.multiple_of(kx * region_y + tile * SUB, SUB), SUB)
                g_ref[node, 0, to, :] = re
                g_ref[node, 1, to, :] = im


def depth_forward(region, box, field_ref, zr, zi, pitch):
    x0, nx, y0, ny = box
    step = max(1, 2 * LANES // ny)
    for x in range(x0, x0 + nx, step):
        count = min(step, x0 + nx - x)
        left = region[pl.ds(x, count), pl.ds(y0, ny), :].reshape(count * ny, LANES)
        both = product(left, field_ref[...])
        for i in range(count):
            zr[pl.ds((x + i) * pitch + y0, ny), :] = both[i * ny : (i + 1) * ny, :LANES]
            zi[pl.ds((x + i) * pitch + y0, ny), :] = both[i * ny : (i + 1) * ny, LANES:]


def blended_columns(
    count_x, count_y, half, g_ref, back_ref, zr, zi, yr, yi, vx, ur, ui, w_ref, o_ref
):
    region_x, region_y = count_x + 2 * half, count_y + 2 * half
    pitch_x, pitch_y = pitch_of(region_x), pitch_of(region_y)

    @pl.loop(0, region_x // SUB)
    def _(tile):
        at = lambda y: pl.ds(tile * SUB * pitch_y + y, SUB, stride=pitch_y)
        values = [(zr[at(y), :], zi[at(y), :]) for y in range(region_y)]
        for ky, (re, im) in enumerate(transform(values, -1, region_y)):
            to = pl.ds(pl.multiple_of(ky * pitch_x + tile * SUB, SUB), SUB)
            yr[to, :] = re
            yi[to, :] = im

    @pl.loop(0, region_y // SUB)
    def _(tile):
        at = lambda x: pl.ds(tile * SUB * pitch_x + x, SUB, stride=pitch_x)
        values = [(yr[at(x), :], yi[at(x), :]) for x in range(region_x)]
        for kx, (re, im) in enumerate(transform(values, -1, region_x)):
            vx[0, kx] = re
            vx[1, kx] = im

        @pl.loop(0, 2)
        def _(j):
            parts = []
            for i in range(2):
                values = []
                for kx in range(region_x):
                    to = pl.ds(pl.multiple_of(kx * region_y + tile * SUB, SUB), SUB)
                    gr, gi = g_ref[2 * j + i, 0, to, :], g_ref[2 * j + i, 1, to, :]
                    vr, vi = vx[0, kx], vx[1, kx]
                    values.append((vr * gr - vi * gi, vr * gi + vi * gr))
                parts.append(transform(values, 1, count_x))
            for x in range(count_x):
                s = (x + 0.5) / count_x
                to = pl.ds(pl.multiple_of(x * pitch_y + tile * SUB, SUB), SUB)
                (ar, ai), (br, bi) = parts[0][x], parts[1][x]
                ur[j, to, :] = (1.0 - s) * ar + s * br
                ui[j, to, :] = (1.0 - s) * ai + s * bi

    @pl.loop(0, count_x // SUB)
    def _(tile):
        parts = []
        for j in range(2):
            at = lambda ky: pl.ds(tile * SUB * pitch_y + ky, SUB, stride=pitch_y)
            values = [(ur[j, at(ky), :], ui[j, at(ky), :]) for ky in range(region_y)]
            parts.append(transform(values, 1, count_y))
        for y in range(count_y):
            t = (y + 0.5) / count_y
            to = pl.ds(pl.multiple_of(y * count_x + tile * SUB, SUB), SUB)
            (ar, ai), (br, bi) = parts[0][y], parts[1][y]
            w_ref[to, :LANES] = (1.0 - t) * ar + t * br
            w_ref[to, LANES:] = (1.0 - t) * ai + t * bi

    o_ref[...] = product(w_ref[...], back_ref[...])


class Link:
    def __init__(self, sems, k, src, dst, axis, by, only=True):
        here, size = lax.axis_index(axis), lax.axis_size(axis)
        inside = lambda i: jnp.logical_and(jnp.logical_and(i >= 0, i < size), only)
        self.sends, self.gets = inside(here + by), inside(here - by)
        self.copy = pltpu.make_async_remote_copy(
            src_ref=src, dst_ref=dst, send_sem=sems[0].at[k], recv_sem=sems[1].at[k],
            device_id={axis: here + by}, device_id_type=pl.DeviceIdType.MESH,
        )

    def start(self):
        pl.when(self.sends)(lambda: self.copy.start())

    def wait_recv(self):
        pl.when(self.gets)(lambda: self.copy.wait_recv())

    def wait_send(self):
        pl.when(self.sends)(lambda: self.copy.wait_send())


def halo_links(region, count_x, count_y, half, sems, base):
    gy, size = lax.axis_index("gy"), lax.axis_size("gy")
    own_x, own_y = pl.ds(half, count_x), pl.ds(half, count_y)
    low, high_x, high_y = pl.ds(0, half), pl.ds(half + count_x, half), pl.ds(half + count_y, half)
    last_x, last_y, first = pl.ds(count_x, half), pl.ds(count_y, half), pl.ds(half, half)
    at = lambda x, y: region.at[x, y]
    along_y = [
        Link(sems, base, at(own_x, last_y), at(own_x, low), "gy", 1),
        Link(sems, base + 1, at(own_x, first), at(own_x, high_y), "gy", -1),
    ]
    along_x = [
        Link(sems, base + 2, at(last_x, own_y), at(low, own_y), "gx", 1),
        Link(sems, base + 3, at(first, own_y), at(high_x, own_y), "gx", -1),
    ]
    relayed = [
        Link(sems, base + 4, at(last_x, low), at(low, low), "gx", 1, gy > 0),
        Link(sems, base + 5, at(first, low), at(high_x, low), "gx", -1, gy > 0),
        Link(sems, base + 6, at(last_x, high_y), at(low, high_y), "gx", 1, gy < size - 1),
        Link(sems, base + 7, at(first, high_y), at(high_x, high_y), "gx", -1, gy < size - 1),
    ]
    return along_y, along_x, relayed


def whole_kernel(
    count_x, count_y, half, rows,
    data_ref, precond_ref, psf_ref, field_ref, kernel_ref, back_ref,
    model_ref, residual_ref,
    region0, region1, nodes, packed, g_ref, k1r, k1i, k2r, k2i,
    zr, zi, yr, yi, vx, ur, ui, w_ref, o_ref, send_sem, recv_sem,
):
    width = 2 * half + 1
    region_x, region_y = count_x + 2 * half, count_y + 2 * half
    pitch_y = pitch_of(region_y)
    sems = (send_sem, recv_sem)
    gx, gy = lax.axis_index("gx"), lax.axis_index("gy")
    size_x, size_y = lax.axis_size("gx"), lax.axis_size("gy")
    regions = [region0, region1]
    for region in regions:
        region[...] = jnp.zeros(region.shape, region.dtype)

    barrier = pltpu.get_barrier_semaphore()
    for axis, here, size in (("gx", gx, size_x), ("gy", gy, size_y)):
        for by in (-1, 1):
            @pl.when(jnp.logical_and(here + by >= 0, here + by < size))
            def _():
                pl.semaphore_signal(
                    barrier, inc=1, device_id={axis: here + by},
                    device_id_type=pl.DeviceIdType.MESH,
                )

    own = (pl.ds(half, count_x), pl.ds(half, count_y))
    region0[own] = precond_ref[...] * data_ref[...]
    peers = 0
    for here, size in ((gx, size_x), (gy, size_y)):
        peers += (here > 0).astype(jnp.int32) + (here < size - 1).astype(jnp.int32)
    pl.semaphore_wait(barrier, peers)

    inline = Link(sems, 16, psf_ref, nodes.at[0], "gx", -1)
    crossline = Link(sems, 17, psf_ref, nodes.at[1], "gy", -1)
    corner = Link(sems, 18, nodes.at[1], nodes.at[2], "gx", -1, gy < size_y - 1)
    crossline.start()
    inline.start()
    started = [crossline, inline, corner]

    for sweep_index in range(ITERS):
        region = regions[sweep_index]
        along_y, along_x, relayed = halo_links(
            region, count_x, count_y, half, sems, 8 * sweep_index
        )
        started += along_y + along_x + relayed
        for link in along_y + along_x:
            link.start()
        depth_forward(region, (half, count_x, half, count_y), field_ref, zr, zi, pitch_y)
        if sweep_index == 0:
            crossline.wait_recv()
            corner.start()
            inline.wait_recv()
            corner.wait_recv()
            last_x, last_y = gx == size_x - 1, gy == size_y - 1
            part = lambda n: pl.ds(n * width, width)

            def fill(n, edge, other, slot):
                @pl.when(edge)
                def _():
                    packed[part(n), :] = packed[part(other), :]

                @pl.when(jnp.logical_not(edge))
                def _():
                    packed[part(n), :] = nodes[slot, pl.ds(0, width), :]

            packed[...] = jnp.zeros(packed.shape, packed.dtype)
            packed[part(0), :] = psf_ref[pl.ds(0, width), :]
            fill(1, last_x, 0, 0)
            fill(2, last_y, 0, 1)

            @pl.when(last_x)
            def _():
                packed[part(3), :] = packed[part(2), :]

            @pl.when(jnp.logical_not(last_x))
            def _():
                fill(3, last_y, 1, 2)

            spectra(
                width, region_x, region_y, rows, packed, kernel_ref, g_ref, k1r, k1i, k2r, k2i
            )
        for link in along_y:
            link.wait_recv()
        for link in relayed:
            link.start()
        depth_forward(region, (half, count_x, 0, half), field_ref, zr, zi, pitch_y)
        depth_forward(region, (half, count_x, half + count_y, half), field_ref, zr, zi, pitch_y)
        for link in along_x + relayed:
            link.wait_recv()
        depth_forward(region, (0, half, 0, region_y), field_ref, zr, zi, pitch_y)
        depth_forward(region, (half + count_x, half, 0, region_y), field_ref, zr, zi, pitch_y)
        blended_columns(
            count_x, count_y, half, g_ref, back_ref, zr, zi, yr, yi, vx, ur, ui, w_ref, o_ref
        )
        last = sweep_index == ITERS - 1
        for x in range(count_x):
            blended = o_ref[pl.ds(x, count_y, stride=count_x), :]
            model = region[x + half, pl.ds(half, count_y), :]
            residual = data_ref[x] - (model + blended)
            model = model + relaxation * precond_ref[x] * residual
            if last:
                residual_ref[x] = residual
                model_ref[x] = model
            else:
                regions[sweep_index + 1][x + half, pl.ds(half, count_y), :] = model
    for link in started:
        link.wait_send()


def local(data, precond, psf):
    count_x, count_y, depth = data.shape
    width = psf.shape[2]
    half = width // 2
    region_x, region_y = count_x + 2 * half, count_y + 2 * half
    pitch_x, pitch_y = pitch_of(region_x), pitch_of(region_y)
    field, kernel, back = tables(depth, width)
    back = back / (region_x * region_y)
    f32 = jnp.float32
    up = lambda n, m: -(-n // m) * m
    flat = psf.reshape(width, width * width)
    high, lanes = up(width, SUB), up(width * width, LANES)
    flat = jnp.pad(flat, ((0, high - width), (0, lanes - width * width)))
    rows = up(4 * width, SUB)
    vmem = lambda *shape: pltpu.VMEM(shape, f32)
    square = region_x * region_y
    spec = pl.BlockSpec(memory_space=pltpu.VMEM)
    model, residual = pl.pallas_call(
        functools.partial(whole_kernel, count_x, count_y, half, rows),
        out_shape=[jax.ShapeDtypeStruct(data.shape, f32)] * 2,
        in_specs=[spec] * 6,
        out_specs=[spec] * 2,
        scratch_shapes=[
            vmem(region_x, region_y, depth),
            vmem(region_x, region_y, depth),
            vmem(3, high, lanes),
            vmem(rows, lanes),
            vmem(4, 2, square, LANES),
            vmem(width * rows, LANES),
            vmem(width * rows, LANES),
            vmem(region_y * rows, LANES),
            vmem(region_y * rows, LANES),
            vmem(region_x * pitch_y, LANES),
            vmem(region_x * pitch_y, LANES),
            vmem(region_y * pitch_x, LANES),
            vmem(region_y * pitch_x, LANES),
            vmem(2, region_x, SUB, LANES),
            vmem(2, count_x * pitch_y, LANES),
            vmem(2, count_x * pitch_y, LANES),
            vmem(count_x * count_y, 2 * LANES),
            vmem(count_x * count_y, LANES),
            pltpu.SemaphoreType.DMA((19,)),
            pltpu.SemaphoreType.DMA((19,)),
        ],
        compiler_params=pltpu.CompilerParams(
            vmem_limit_bytes=32 << 20, collective_id=0, has_side_effects=True
        ),
        name="whole",
    )(data, precond, flat, stacked(field), stacked(kernel), stacked(back))
    return model, residual


def solution(mesh):
    placed = (P("gx", "gy", None), P("gx", "gy", None), P("gx", "gy", None, None, None))
    return jax.shard_map(
        local,
        mesh=mesh,
        in_specs=placed,
        out_specs=(P("gx", "gy", None), P("gx", "gy", None)),
        check_vma=False,
    )
```
